32 devices in a mesh: batch: 16 (over z, y, x), cols: 2 (over core).
Axes of the slice: x: 2, y: 2, z: 4, core: 2. Of those that a mesh axis runs over, the one named last changes fastest.
Arguments:
- grad_up: float32 [16, 1024, 4096], P('batch', None, 'cols'), may hold values from -0.875 to 0.875
- grad_down: float32 [16, 4096, 1024], P('batch', 'cols'), may hold values from -0.875 to 0.875
- grad_query: float32 [16, 1024, 1024], P('batch', None, 'cols'), may hold values from -0.875 to 0.875
- grad_key: float32 [16, 1024, 1024], P('batch', None, 'cols'), may hold values from -0.875 to 0.875
- grad_value: float32 [16, 1024, 1024], P('batch', None, 'cols'), may hold values from -0.875 to 0.875
- grad_mixed: float32 [16, 1024, 1024], P('batch', 'cols'), may hold values from -0.875 to 0.875
- grad_norm: float32 [16, 1024], P('batch'), may hold values from -8 to 8
- weight_up: float32 [1024, 4096], P('batch', 'cols'), may hold values from -0.1875 to 0.1875
- weight_down: float32 [4096, 1024], P('cols', 'batch'), may hold values from -0.09375 to 0.09375
- weight_query: float32 [1024, 1024], P('batch', 'cols'), may hold values from -0.1875 to 0.1875
- weight_key: float32 [1024, 1024], P('batch', 'cols'), may hold values from -0.1875 to 0.1875
- weight_value: float32 [1024, 1024], P('batch', 'cols'), may hold values from -0.1875 to 0.1875
- weight_mixed: float32 [1024, 1024], P('cols', 'batch'), may hold values from -0.1875 to 0.1875
- weight_norm: float32 [1024], P('batch'), may hold values from 0.25 to 1.75
Outputs:
- copy_up: bfloat16 [1024, 4096], P(None, 'cols')
- copy_down: bfloat16 [4096, 1024], P('cols')
- copy_query: bfloat16 [1024, 1024], P(None, 'cols')
- copy_key: bfloat16 [1024, 1024], P(None, 'cols')
- copy_value: bfloat16 [1024, 1024], P(None, 'cols')
- copy_mixed: bfloat16 [1024, 1024], P('cols')
- copy_norm: bfloat16 [1024], replicated
- new_up: float32 [1024, 4096], P('batch', 'cols')
- new_down: float32 [4096, 1024], P('cols', 'batch')
- new_query: float32 [1024, 1024], P('batch', 'cols')
- new_key: float32 [1024, 1024], P('batch', 'cols')
- new_value: float32 [1024, 1024], P('batch', 'cols')
- new_mixed: float32 [1024, 1024], P('cols', 'batch')
- new_norm: float32 [1024], P('batch')
The draws below stay inside these ranges and needn't reach their ends.
All inputs are finite; a program needn't handle non-finite values.
Results may differ from the reference program's by a relative error of at most 0.0004.
Values may be sent and summed in bfloat16 or wider, within the bound.
A program may use at most 128 MiB of HBM per device.

```python
import jax
import jax.numpy as jnp

WIDTH = 1024
INNER = 4096
ATTN = 1024
REPLICAS = 16


def strengthened(array, own_key, source, target, blocks, factor):
    def block_of(dim):
        return (jnp.arange(array.shape[dim]) // (array.shape[dim] // blocks)).reshape((-1,) + (1,) * (array.ndim - 1 - dim))

    first = jax.random.permutation(own_key, blocks)[block_of(target)]
    far = (block_of(target) + blocks // 2) % blocks
    return jnp.where((block_of(source) == first) | (block_of(source) == far), factor * array, array)


def shard_levels(key, dims, cuts, least, top_value):
    def one(position, shards_of):
        steps = jax.random.uniform(jax.random.fold_in(jax.random.fold_in(key, 6), position), (shards_of,), jnp.float32, least / len(cuts), top_value / len(cuts))
        return jnp.repeat(jnp.exp(steps), dims[position] // shards_of).reshape((-1,) + (1,) * (len(dims) - position - 1))

    loudness = one(*cuts[0])
    for cut in cuts[1:]:
        loudness = loudness * one(*cut)
    return loudness


def gaussian(stream_key, dims, width, limit, pieces=(), dtype=jnp.bfloat16):
    factor_of = shard_levels(stream_key, dims, pieces, -0.22, 0.18) if pieces else 1.0
    result = jax.random.normal(stream_key, dims, jnp.float32) * width * factor_of
    return jnp.minimum(jnp.maximum(result, -limit), limit).astype(dtype)


def noise_with(own_key, shape, spread, reach, cuts, heavy, held_as=jnp.bfloat16):
    array = spread * jax.random.normal(own_key, shape, jnp.float32)
    if cuts:
        array = array * shard_levels(own_key, shape, cuts, -0.22, 0.18)
    return jnp.clip(strengthened(array, jax.random.fold_in(own_key, 3), *heavy), -reach, reach).astype(held_as)


def setup_inputs(seed: int = 0) -> dict:
    key_of = jax.random.split(jax.random.key(seed), 15)
    grad_up = noise_with(key_of[0], (REPLICAS, WIDTH, INNER), 0.1, 0.875, ((0, 16), (2, 2)), (0, 1, 16, 2.0), jnp.float32)
    grad_down = noise_with(key_of[1], (REPLICAS, INNER, WIDTH), 0.1, 0.875, ((0, 16), (1, 2)), (0, 2, 16, 2.0), jnp.float32)
    grad_query = noise_with(key_of[2], (REPLICAS, WIDTH, ATTN), 0.1, 0.875, ((0, 16), (2, 2)), (0, 1, 16, 2.0), jnp.float32)
    grad_key = noise_with(key_of[3], (REPLICAS, WIDTH, ATTN), 0.1, 0.875, ((0, 16), (2, 2)), (0, 1, 16, 2.0), jnp.float32)
    grad_value = noise_with(key_of[4], (REPLICAS, WIDTH, ATTN), 0.1, 0.875, ((0, 16), (2, 2)), (0, 1, 16, 2.0), jnp.float32)
    grad_mixed = noise_with(key_of[5], (REPLICAS, ATTN, WIDTH), 0.1, 0.875, ((0, 16), (1, 2)), (0, 2, 16, 2.0), jnp.float32)
    grad_norm = noise_with(key_of[6], (REPLICAS, WIDTH), 1.0, 8.0, ((0, 16),), (0, 1, 16, 2.0), jnp.float32)
    weight_up = gaussian(key_of[7], (WIDTH, INNER), WIDTH ** -0.5, 0.1875, ((0, 16), (1, 2)), jnp.float32)
    weight_down = gaussian(key_of[8], (INNER, WIDTH), INNER ** -0.5, 0.09375, ((0, 2), (1, 16)), jnp.float32)
    weight_query = gaussian(key_of[9], (WIDTH, ATTN), WIDTH ** -0.5, 0.1875, ((0, 16), (1, 2)), jnp.float32)
    weight_key = gaussian(key_of[10], (WIDTH, ATTN), WIDTH ** -0.5, 0.1875, ((0, 16), (1, 2)), jnp.float32)
    weight_value = gaussian(key_of[11], (WIDTH, ATTN), WIDTH ** -0.5, 0.1875, ((0, 16), (1, 2)), jnp.float32)
    weight_mixed = gaussian(key_of[12], (ATTN, WIDTH), ATTN ** -0.5, 0.1875, ((0, 2), (1, 16)), jnp.float32)
    weight_norm = jnp.clip(1.0 + 0.15 * jax.random.normal(key_of[13], (WIDTH,), jnp.float32), 0.25, 1.75)
    return {"grad_up": grad_up, "grad_down": grad_down, "grad_query": grad_query, "grad_key": grad_key, "grad_value": grad_value, "grad_mixed": grad_mixed, "grad_norm": grad_norm, "weight_up": weight_up, "weight_down": weight_down, "weight_query": weight_query, "weight_key": weight_key, "weight_value": weight_value, "weight_mixed": weight_mixed, "weight_norm": weight_norm}


learn_rate = 0.3


def reference(grad_up, grad_down, grad_query, grad_key, grad_value, grad_mixed, grad_norm, weight_up, weight_down, weight_query, weight_key, weight_value, weight_mixed, weight_norm):
    mean_up = jnp.sum(grad_up.astype(jnp.float32), axis=0) * REPLICAS ** -0.5
    mean_down = jnp.sum(grad_down.astype(jnp.float32), axis=0) * REPLICAS ** -0.5
    mean_query = jnp.sum(grad_query.astype(jnp.float32), axis=0) * REPLICAS ** -0.5
    mean_key = jnp.sum(grad_key.astype(jnp.float32), axis=0) * REPLICAS ** -0.5
    mean_value = jnp.sum(grad_value.astype(jnp.float32), axis=0) * REPLICAS ** -0.5
    mean_mixed = jnp.sum(grad_mixed.astype(jnp.float32), axis=0) * REPLICAS ** -0.5
    mean_norm = jnp.sum(grad_norm.astype(jnp.float32), axis=0) * REPLICAS ** -0.5
    new_up = weight_up - learn_rate * mean_up
    new_down = weight_down - learn_rate * mean_down
    new_query = weight_query - learn_rate * mean_query
    new_key = weight_key - learn_rate * mean_key
    new_value = weight_value - learn_rate * mean_value
    new_mixed = weight_mixed - learn_rate * mean_mixed
    new_norm = weight_norm - learn_rate * mean_norm
    copy_up = new_up.astype(jnp.bfloat16)
    copy_down = new_down.astype(jnp.bfloat16)
    copy_query = new_query.astype(jnp.bfloat16)
    copy_key = new_key.astype(jnp.bfloat16)
    copy_value = new_value.astype(jnp.bfloat16)
    copy_mixed = new_mixed.astype(jnp.bfloat16)
    copy_norm = new_norm.astype(jnp.bfloat16)
    return copy_up, copy_down, copy_query, copy_key, copy_value, copy_mixed, copy_norm, new_up, new_down, new_query, new_key, new_value, new_mixed, new_norm
```

```python
import jax
import jax.numpy as jnp
from jax import lax
from jax.sharding import PartitionSpec as P

learn_rate = 0.3
PIECES = 2


def half(array, axis, inner, which):
    outer = array.shape[axis] // (2 * inner)
    if outer == 1:
        return lax.dynamic_slice_in_dim(array, which * inner, inner, axis)
    if axis == 0:
        split = array.reshape((outer, 2, inner) + array.shape[1:])
        return lax.dynamic_index_in_dim(split, which, 1, False).reshape((outer * inner,) + array.shape[1:])
    return jnp.concatenate(
        [lax.dynamic_slice_in_dim(array, (2 * i + which) * inner, inner, axis) for i in range(outer)], axis
    )


def merged(own, other, axis, inner, which):
    first = jnp.where(which == 0, own, other)
    second = jnp.where(which == 0, other, own)
    outer = own.shape[axis] // inner
    if axis == 0:
        rest = own.shape[1:]
        pair = [a.reshape((outer, 1, inner) + rest) for a in (first, second)]
        return jnp.concatenate(pair, 1).reshape((2 * outer * inner,) + rest)
    parts = []
    for i in range(outer):
        parts += [lax.slice_in_dim(a, i * inner, (i + 1) * inner, axis=axis) for a in (first, second)]
    return jnp.concatenate(parts, axis)


def swap(array, bit, size):
    pairs = [(i, i ^ (1 << bit)) for i in range(size)]
    rows, columns = array.shape
    folds = 128 // columns if columns < 128 else 1
    if folds > 1 and rows % (folds * 16) == 0:
        tall = rows // folds
        wide = jnp.concatenate([array[i * tall : (i + 1) * tall] for i in range(folds)], 1)
        wide = lax.ppermute(wide, "batch", pairs)
        return jnp.concatenate([wide[:, i * columns : (i + 1) * columns] for i in range(folds)], 0)
    return lax.ppermute(array, "batch", pairs)


def inner_of(bit, left, unit):
    return unit << sum(1 for other in left if other < bit)


def reduced(grad, axis, order, size):
    unit = grad.shape[axis] // size
    me = lax.axis_index("batch")
    left = set(order)
    for bit in order:
        mine = (me >> bit) & 1
        inner = inner_of(bit, left, unit)
        other = swap(half(grad, axis, inner, 1 - mine), bit, size)
        grad = half(grad, axis, inner, mine) + other
        left.discard(bit)
    return grad


def spread(own, axis, order, size):
    unit = own.shape[axis]
    me = lax.axis_index("batch")
    left = set()
    for bit in reversed(order):
        mine = (me >> bit) & 1
        inner = inner_of(bit, left, unit)
        own = merged(own, swap(own, bit, size), axis, inner, mine)
        left.add(bit)
    return own


def shards(*arrays):
    count = len(arrays) // 2
    grads, weights = arrays[:count], arrays[count:]
    size = lax.axis_size("batch")
    bits = size.bit_length() - 1
    rate = learn_rate * size ** (-0.5)
    straight = list(range(bits))
    late = [0] + straight[2:] + [1]
    turned = straight[1:] + [0]
    plan = ((0, straight, PIECES), (1, turned, PIECES), (0, late, 1), (0, late, 1), (0, late, 1), (1, turned, 1))
    copies, news = [], []
    for grad, weight, (axis, order, pieces) in zip(grads, weights, plan):
        cut = 1 - axis
        wide = weight.shape[cut] // pieces
        copy, new = [], []
        for i in range(pieces):
            part = lax.slice_in_dim(grad[0], i * wide, (i + 1) * wide, axis=cut)
            total = reduced(part, axis, order, size)
            value = lax.slice_in_dim(weight, i * wide, (i + 1) * wide, axis=cut) - rate * total
            new.append(value)
            copy.append(spread(value.astype(jnp.bfloat16), axis, order, size))
        copies.append(jnp.concatenate(copy, cut) if pieces > 1 else copy[0])
        news.append(jnp.concatenate(new, cut) if pieces > 1 else new[0])
    total = reduced(grads[-1].reshape(size, -1), 0, straight, size)
    value = weights[-1].reshape(1, -1) - rate * total
    news.append(value.reshape(-1))
    copies.append(spread(value.astype(jnp.bfloat16), 0, straight, size).reshape(-1))
    return tuple(copies) + tuple(news)


def solution(mesh):
    rows, columns = P("batch", "cols"), P("cols", "batch")
    return jax.shard_map(
        shards,
        mesh=mesh,
        in_specs=(
            P("batch", None, "cols"),
            P("batch", "cols", None),
            P("batch", None, "cols"),
            P("batch", None, "cols"),
            P("batch", None, "cols"),
            P("batch", "cols", None),
            P("batch", None),
            rows,
            columns,
            rows,
            rows,
            rows,
            columns,
            P("batch"),
        ),
        out_specs=(
            P(None, "cols"),
            P("cols", None),
            P(None, "cols"),
            P(None, "cols"),
            P(None, "cols"),
            P("cols", None),
            P(),
            rows,
            columns,
            rows,
            rows,
            rows,
            columns,
            P("batch"),
        ),
        check_vma=False,
    )
```

```python
import functools

import jax
import jax.numpy as jnp
from jax import lax
from jax.experimental import pallas as pl
from jax.experimental.pallas import tpu as pltpu
from jax.sharding import PartitionSpec as P

learn_rate = 0.3
PIECES = 2


def half(array, axis, inner, which):
    outer = array.shape[axis] // (2 * inner)
    if outer == 1:
        return lax.dynamic_slice_in_dim(array, which * inner, inner, axis)
    if axis == 0:
        split = array.reshape((outer, 2, inner) + array.shape[1:])
        return lax.dynamic_index_in_dim(split, which, 1, False).reshape((outer * inner,) + array.shape[1:])
    return jnp.concatenate(
        [lax.dynamic_slice_in_dim(array, (2 * i + which) * inner, inner, axis) for i in range(outer)], axis
    )


def merged(own, other, axis, inner, which):
    first = jnp.where(which == 0, own, other)
    second = jnp.where(which == 0, other, own)
    outer = own.shape[axis] // inner
    if axis == 0:
        rest = own.shape[1:]
        pair = [a.reshape((outer, 1, inner) + rest) for a in (first, second)]
        return jnp.concatenate(pair, 1).reshape((2 * outer * inner,) + rest)
    parts = []
    for i in range(outer):
        parts += [lax.slice_in_dim(a, i * inner, (i + 1) * inner, axis=axis) for a in (first, second)]
    return jnp.concatenate(parts, axis)


def swap(array, bit, size):
    pairs = [(i, i ^ (1 << bit)) for i in range(size)]
    rows, columns = array.shape
    folds = 128 // columns if columns < 128 else 1
    if folds > 1 and rows % (folds * 16) == 0:
        tall = rows // folds
        wide = jnp.concatenate([array[i * tall : (i + 1) * tall] for i in range(folds)], 1)
        wide = lax.ppermute(wide, "batch", pairs)
        return jnp.concatenate([wide[:, i * columns : (i + 1) * columns] for i in range(folds)], 0)
    return lax.ppermute(array, "batch", pairs)


def inner_of(bit, left, unit):
    return unit << sum(1 for other in left if other < bit)


def reduced(grad, axis, order, size):
    unit = grad.shape[axis] // size
    me = lax.axis_index("batch")
    left = set(order)
    for bit in order:
        mine = (me >> bit) & 1
        inner = inner_of(bit, left, unit)
        other = swap(half(grad, axis, inner, 1 - mine), bit, size)
        grad = half(grad, axis, inner, mine) + other
        left.discard(bit)
    return grad


def spread(own, axis, order, size):
    unit = own.shape[axis]
    me = lax.axis_index("batch")
    left = set()
    for bit in reversed(order):
        mine = (me >> bit) & 1
        inner = inner_of(bit, left, unit)
        own = merged(own, swap(own, bit, size), axis, inner, mine)
        left.add(bit)
    return own


def by_permutes(grads, weights, size):
    bits = size.bit_length() - 1
    rate = learn_rate * size ** (-0.5)
    straight = list(range(bits))
    late = [0] + straight[2:] + [1]
    turned = straight[1:] + [0]
    plan = ((0, straight, PIECES), (1, turned, PIECES), (0, late, 1), (0, late, 1), (0, late, 1), (1, turned, 1))
    copies, news = [], []
    for grad, weight, (axis, order, pieces) in zip(grads, weights, plan):
        cut = 1 - axis
        wide = weight.shape[cut] // pieces
        copy, new = [], []
        for i in range(pieces):
            part = lax.slice_in_dim(grad[0], i * wide, (i + 1) * wide, axis=cut)
            total = reduced(part, axis, order, size)
            value = lax.slice_in_dim(weight, i * wide, (i + 1) * wide, axis=cut) - rate * total
            new.append(value)
            copy.append(spread(value.astype(jnp.bfloat16), axis, order, size))
        copies.append(jnp.concatenate(copy, cut) if pieces > 1 else copy[0])
        news.append(jnp.concatenate(new, cut) if pieces > 1 else new[0])
    total = reduced(grads[-1].reshape(size, -1), 0, straight, size)
    value = weights[-1].reshape(1, -1) - rate * total
    news.append(value.reshape(-1))
    copies.append(spread(value.astype(jnp.bfloat16), 0, straight, size).reshape(-1))
    return tuple(copies) + tuple(news)


def kernel(size, rate, wide, tall, *refs):
    g_up, g_down, g_query, g_key, g_value, g_mixed, share = refs[:7]
    w_up, w_down, w_query, w_key, w_value, w_mixed = refs[7:13]
    c_up, c_down, c_query, c_key, c_value, c_mixed, norm = refs[13:20]
    n_up, n_down, n_query, n_key, n_value, n_mixed = refs[20:26]
    acc_u, u1, u2, u3, u4, own_u, acc_d, d1, d2, d3, d4, own_d, far_d, full_d, ring, send, recv, local = refs[26:]
    me = lax.axis_index("batch")
    bit = [(me // 2**b) % 2 for b in range(4)]
    peer = [me + (1 - 2 * bit[b]) * 2**b for b in range(4)]

    barrier = pltpu.get_barrier_semaphore()
    for b in range(4):
        pl.semaphore_signal(barrier, inc=1, device_id={"batch": peer[b]}, device_id_type=pl.DeviceIdType.MESH)
    pl.semaphore_wait(barrier, 4)

    sent, used = [], [0, 0]

    def push(source, target, b):
        copy = pltpu.make_async_remote_copy(
            src_ref=source,
            dst_ref=target,
            send_sem=send.at[used[0]],
            recv_sem=recv.at[used[0]],
            device_id={"batch": peer[b]},
            device_id_type=pl.DeviceIdType.MESH,
        )
        used[0] += 1
        copy.start()
        sent.append(copy)
        return copy

    def place(source, target):
        copy = pltpu.make_async_copy(source, target, local.at[used[1]])
        used[1] += 1
        copy.start()
        return copy

    def rows_stream(s, grad, weight, copy_out, new_out, at, order):
        cols = pl.ds(at, wide)
        boxes = (u1, u2, u3, u4)
        every = slice(None)
        going = push(grad.at[:, :, :, 1 - bit[0], :, cols], u1.at[s], 0)
        held = place(grad.at[:, :, :, bit[0], :, cols], acc_u.at[s])
        yield
        held.wait()
        done = {0}
        for stage in range(4):
            going.wait_recv()
            left = [b for b in (3, 2, 1) if b not in done]

            def add(i, _, left=left, box=boxes[stage], done=done):
                digit = {b: (i // 2 ** (len(left) - 1 - k)) % 2 for k, b in enumerate(left)}
                spot = (s,) + tuple(digit.get(b, bit[b]) for b in (3, 2, 1))
                acc_u[spot] = acc_u[spot] + box[(s,) + tuple(digit[b] for b in left)]
                return 0

            lax.fori_loop(0, 2 ** len(left), add, 0)
            if stage < 3:
                b = order[stage + 1]
                spot = tuple(1 - bit[c] if c == b else bit[c] if c in done else every for c in (3, 2, 1))
                going = push(acc_u.at[(s,) + spot], boxes[stage + 1].at[s], b)
                done = done | {b}
                yield
        value = weight[:, cols] - rate * acc_u[s, bit[3], bit[2], bit[1]]
        new_out[:, cols] = value
        own_u[s] = value.astype(jnp.bfloat16)
        mine = copy_out.at[bit[3], bit[2], bit[1], bit[0], :, cols]
        held = place(own_u.at[s], mine)
        going = push(own_u.at[s], mine, order[3])
        have = {order[3]}
        yield
        held.wait()
        for b in order[2::-1]:
            going.wait_recv()
            spot = tuple(every if c in have else bit[c] for c in (3, 2, 1, 0)) + (every, cols)
            going = push(copy_out.at[spot], copy_out.at[spot], b)
            have = have | {b}
            yield
        going.wait_recv()
        yield

    def columns_stream(s, grad, weight, copy_out, new_out, at):
        rows = pl.ds(at, tall)
        pairs = [(a, c) for a in range(2) for c in range(2)]

        def block(z2, z1, y):
            return (rows, pl.ds(pl.multiple_of((z2 * 4 + z1 * 2 + y) * 128, 128), 128))

        going = [push(grad.at[block(a, c, 1 - bit[1])], d1.at[s, a, c], 1) for a, c in pairs]
        held = [place(grad.at[block(a, c, bit[1])], acc_d.at[s, a, c]) for a, c in pairs]
        yield
        for copy in held:
            copy.wait()
        for copy in going:
            copy.wait_recv()

        def add1(i, _):
            acc_d[s, i // 2, i % 2] = acc_d[s, i // 2, i % 2] + d1[s, i // 2, i % 2]
            return 0

        lax.fori_loop(0, 4, add1, 0)
        going = push(acc_d.at[s, :, 1 - bit[2]], d2.at[s], 2)
        yield
        going.wait_recv()

        def add2(i, _):
            acc_d[s, i, bit[2]] = acc_d[s, i, bit[2]] + d2[s, i]
            return 0

        lax.fori_loop(0, 2, add2, 0)
        going = push(acc_d.at[s, 1 - bit[3], bit[2]], d3.at[s], 3)
        yield
        going.wait_recv()
        acc_d[s, bit[3], bit[2]] = acc_d[s, bit[3], bit[2]] + d3[s]
        going = push(acc_d.at[s, bit[3], bit[2]], d4.at[s], 0)
        yield
        going.wait_recv()
        total = acc_d[s, bit[3], bit[2]] + d4[s]
        part = jnp.where(bit[0] == 0, total[:, :64], total[:, 64:])
        value = weight[rows, :] - rate * part
        new_out[rows, :] = value
        own_d[s] = jnp.concatenate([value, value], 1).astype(jnp.bfloat16)
        going = push(own_d.at[s], far_d.at[s], 0)
        yield
        going.wait_recv()
        lane = lax.broadcasted_iota(jnp.int32, (tall, 128), 1)
        keep = (lane // 64) == bit[0]
        full = jnp.where(keep, own_d[s].astype(jnp.float32), far_d[s].astype(jnp.float32))
        full_d[s] = full.astype(jnp.bfloat16)
        mine = copy_out.at[block(bit[3], bit[2], bit[1])]
        held = place(full_d.at[s], mine)
        going = push(full_d.at[s], mine, 3)
        yield
        held.wait()
        going.wait_recv()
        spots = [copy_out.at[block(a, bit[2], bit[1])] for a in range(2)]
        going = [push(spot, spot, 2) for spot in spots]
        yield
        for copy in going:
            copy.wait_recv()
        spots = [copy_out.at[block(a, c, bit[1])] for a, c in pairs]
        going = [push(spot, spot, 1) for spot in spots]
        yield
        for copy in going:
            copy.wait_recv()
        yield

    def norm_stream():
        ring[0] = share[...]
        for b in range(4):
            going = push(ring.at[b], ring.at[5 + b], b)
            yield
            going.wait_recv()
            ring[b + 1] = ring[b] + ring[5 + b]
        norm[...] = ring[4]
        yield

    straight, late = (0, 1, 2, 3), (0, 2, 3, 1)
    ups = [(g_up, w_up, c_up, n_up, i * wide, straight) for i in range(g_up.shape[-1] // wide)]
    heads = [
        (g_query, w_query, c_query, n_query, 0, late),
        (g_key, w_key, c_key, n_key, 0, late),
        (g_value, w_value, c_value, n_value, 0, late),
    ]
    downs = [(g_down, w_down, c_down, n_down, i * tall) for i in range(g_down.shape[0] // tall)]
    downs.append((g_mixed, w_mixed, c_mixed, n_mixed, 0))
    rows_order = []
    while ups or heads:
        rows_order += heads[:1] + ups[:1]
        heads, ups = heads[1:], ups[1:]
    us = [rows_stream(s, *case) for s, case in enumerate(rows_order)]
    ds = [columns_stream(s, *case) for s, case in enumerate(downs)]
    live = []
    waves = [norm_stream()]
    for s in range(max(len(us), len(ds))):
        live.append(us[s : s + 1] + ds[s : s + 1])
    live[0] = waves + live[0]
    ahead = 2
    for slot in range(len(live) + 9):
        if slot == 0:
            for wave in live[:ahead]:
                for stream in wave:
                    next(stream, None)
        elif slot + ahead - 1 < len(live):
            for stream in live[slot + ahead - 1]:
                next(stream, None)
        for wave in live[:slot] if slot else []:
            for stream in wave:
                next(stream, None)
    for copy in sent:
        copy.wait_send()


def by_kernel(grads, weights, size):
    rate = learn_rate * size ** (-0.5)
    me = lax.axis_index("batch")
    wide, tall = weights[2].shape[1], weights[5].shape[0]
    share = weights[-1].shape[0]
    base = jnp.zeros((grads[-1].shape[1],), jnp.float32)
    norm = lax.dynamic_update_slice(base, weights[-1], (me * share,)) - rate * grads[-1][0]

    def split(array):
        rows = array.shape[0] // size
        return array.reshape(2, 2, 2, 2, rows, array.shape[1])

    by_rows = (True, False, True, True, True, False)
    ins = [split(g[0]) if r else g[0] for g, r in zip(grads, by_rows)]
    us = ins[0].shape[-1] // wide + 3
    ds = ins[1].shape[0] // tall + 1
    unit = ins[0].shape[-2]
    f32, bf16 = jnp.float32, jnp.bfloat16
    hbm, vmem = pl.BlockSpec(memory_space=pl.ANY), pl.BlockSpec(memory_space=pltpu.VMEM)
    outs = [jax.ShapeDtypeStruct(i.shape, bf16) for i in ins]
    outs += [jax.ShapeDtypeStruct((norm.shape[0] // 128, 128), f32)]
    outs += [jax.ShapeDtypeStruct(w.shape, f32) for w in weights[:6]]
    count = 8 * us + 15 * ds + 4
    results = pl.pallas_call(
        functools.partial(kernel, size, rate, wide, tall),
        out_shape=outs,
        in_specs=[hbm] * 6 + [vmem] * 7,
        out_specs=[hbm] * 6 + [vmem] * 7,
        scratch_shapes=[
            pltpu.VMEM((us, 2, 2, 2, unit, wide), f32),
            pltpu.VMEM((us, 2, 2, 2, unit, wide), f32),
            pltpu.VMEM((us, 2, 2, unit, wide), f32),
            pltpu.VMEM((us, 2, unit, wide), f32),
            pltpu.VMEM((us, unit, wide), f32),
            pltpu.VMEM((us, unit, wide), bf16),
            pltpu.VMEM((ds, 2, 2, tall, 128), f32),
            pltpu.VMEM((ds, 2, 2, tall, 128), f32),
            pltpu.VMEM((ds, 2, tall, 128), f32),
            pltpu.VMEM((ds, tall, 128), f32),
            pltpu.VMEM((ds, tall, 128), f32),
            pltpu.VMEM((ds, tall, 128), bf16),
            pltpu.VMEM((ds, tall, 128), bf16),
            pltpu.VMEM((ds, tall, 128), bf16),
            pltpu.VMEM((9, norm.shape[0] // 128, 128), f32),
            pltpu.SemaphoreType.DMA((count,)),
            pltpu.SemaphoreType.DMA((count,)),
            pltpu.SemaphoreType.DMA((2 * us + 5 * ds,)),
        ],
        compiler_params=pltpu.CompilerParams(
            collective_id=0, has_side_effects=True, vmem_limit_bytes=60 * 1024 * 1024
        ),
    )(*ins, norm.reshape(-1, 128), *weights[:6])
    copies = [c.reshape(g.shape[1:]) for c, g in zip(results[:6], grads)]
    value = results[6].reshape(-1)
    copies.append(value.astype(bf16))
    return tuple(copies) + tuple(results[7:]) + (lax.dynamic_slice(value, (me * share,), (share,)),)


def shards(*arrays):
    count = len(arrays) // 2
    grads, weights = arrays[:count], arrays[count:]
    size = lax.axis_size("batch")
    if size == 16 and 2 * weights[1].shape[1] == 128:
        return by_kernel(grads, weights, size)
    return by_permutes(grads, weights, size)


def solution(mesh):
    rows, columns = P("batch", "cols"), P("cols", "batch")
    return jax.shard_map(
        shards,
        mesh=mesh,
        in_specs=(
            P("batch", None, "cols"),
            P("batch", "cols", None),
            P("batch", None, "cols"),
            P("batch", None, "cols"),
            P("batch", None, "cols"),
            P("batch", "cols", None),
            P("batch", None),
            rows,
            columns,
            rows,
            rows,
            rows,
            columns,
            P("batch"),
        ),
        out_specs=(
            P(None, "cols"),
            P("cols", None),
            P(None, "cols"),
            P(None, "cols"),
            P(None, "cols"),
            P("cols", None),
            P(),
            rows,
            columns,
            rows,
            rows,
            rows,
            columns,
            P("batch"),
        ),
        check_vma=False,
    )
```
